256 devices in a mesh: grid: 2 (over core), px: 16 (over y, x), py: 8 (over z).
Axes of the slice: x: 4, y: 4, z: 8, core: 2. Of those that a mesh axis runs over, the one named last changes fastest.
Arguments:
- residual: float32 [2, 128, 64, 5, 1024], P('grid', 'px', 'py'), may hold values from -3 to 3
- inverses: float32 [2, 128, 64, 25, 1024], P('grid', 'px', 'py'), may hold values from 0 to 1, as said below
- couplings: float32 [2, 128, 64, 4, 1024], P('grid', 'px', 'py'), may hold values from 0.22 to 0.735, as said below
- receptors: int32 [2, 16, 8, 512], P('grid', 'px', 'py'), may hold values from 0 to 65535, as said below
- owners: int32 [2, 16, 8, 512, 1], P('grid', 'px', 'py'), may hold values from 0 to 127; in each aligned block of 512 rows (0 to 511, 512 to 1023, ..., all dimensions but the last counted through in order) at most 8 rows name the same one
- donors: int32 [2, 16, 8, 512, 8], P('grid', 'px', 'py'), may hold values from 0 to 65535
- weights: float32 [2, 16, 8, 512, 8], P('grid', 'px', 'py'), may hold values from 0 to 1, as said below
Outputs:
- update: float32 [2, 128, 64, 5, 1024], P('grid', 'px', 'py')
The draws below stay inside these ranges and needn't reach their ends.
Inputs may be any that keep to these rules, and one draw needn't show every extreme that they name: `receptors`: receptor indices of one device are distinct. `owners`: among the receptors of one device no owner appears more than 8 times, and in every draw some device names one owner exactly 8 times. `weights`: nonnegative; the 8 weights of a receptor sum to 1. `inverses`: all entries nonnegative; off-diagonal entries 0.02 to 0.07; each row of a block sums to 0.94 to 1. `couplings`: a + b and e + f of each cell lie in 0.88 to 0.98, and each coupling is a quarter to three quarters of its pair's sum.
All inputs are finite; a program needn't handle non-finite values.
Results may differ from the reference program's by a relative error of at most 0.0001.
Values sent between devices are 32-bit elements; how exact they have to be, the bound alone decides.
No kernel may reach another device: no remote copies, remote signals or barrier semaphores. Data moves between devices by JAX's collectives and lax.ppermute only.
A program may use at most 128 MiB of HBM per device.

```python
import math
import jax
import jax.numpy as jnp
import numpy as np
from jax import lax

COMPS = 5
DONORS = 8
CI = 8
CJ = 8
CK = 1024
R_DEV = 512
GRIDS = 2
BLOCKS_I = 16
BLOCKS_J = 8
NI = 128
NJ = 64
CELLS = 65536
OWNERS = 128
SLOTS = 8


def draw_residual(key, part):
    shape = (GRIDS, NI, NJ, COMPS, CK)
    return jnp.clip(0.5 * jax.random.normal(key, shape, jnp.float32), -3.0, 3.0)


def draw_inverses(key, part):
    first, second = jax.random.split(key)
    shape = (GRIDS, NI, NJ, COMPS, COMPS, CK)
    row_total = jax.random.uniform(first, (GRIDS, NI, NJ, COMPS, 1, CK), jnp.float32, 0.94, 1.0)
    identity = jnp.eye(COMPS, dtype=jnp.float32).reshape(1, 1, 1, COMPS, COMPS, 1)
    offdiag = jax.random.uniform(second, shape, jnp.float32, 0.02, 0.07) * (1.0 - identity)
    diagonal = row_total - jnp.sum(offdiag, axis=4, keepdims=True)
    blocks = offdiag + identity * diagonal
    return blocks.reshape(GRIDS, NI, NJ, COMPS * COMPS, CK)


def draw_couplings(key, part):
    keys = jax.random.split(key, 4)
    shape = (GRIDS, NI, NJ, 1, CK)
    low_total = 0.88
    lower_total = jax.random.uniform(keys[0], shape, jnp.float32, low_total, 0.98)
    upper_total = jax.random.uniform(keys[1], shape, jnp.float32, low_total, 0.98)
    lower_split = jax.random.uniform(keys[2], shape, jnp.float32, 0.25, 0.75)
    upper_split = jax.random.uniform(keys[3], shape, jnp.float32, 0.25, 0.75)
    return jnp.concatenate([lower_total * lower_split, lower_total * (1.0 - lower_split), upper_total * upper_split, upper_total * (1.0 - upper_split)], axis=3)


def draw_weights(key, part):
    shape = (GRIDS, NI // CI, NJ // CJ, R_DEV, DONORS)
    raw_weight = jax.random.uniform(key, shape, jnp.float32, 0.05, 1.0)
    return raw_weight / jnp.sum(raw_weight, axis=-1, keepdims=True)


def draw_receptors(key, part):
    stride = CELLS // R_DEV
    shape = (GRIDS, NI // CI, NJ // CJ, R_DEV)
    offsets = jax.random.randint(key, shape, 0, stride, dtype=jnp.int32)
    return offsets + jnp.arange(R_DEV, dtype=jnp.int32) * stride


def plant(values, rng, smallest, high):
    index_at = [jax.random.randint(jax.random.fold_in(rng, axis), (), 0, length) for axis, length in enumerate(values.shape)]
    widest = values.shape.index(max(values.shape))
    beside = index_at[:widest] + [(index_at[widest] + 1) % values.shape[widest]] + index_at[widest + 1:]
    return values.at[tuple(index_at)].set(smallest).at[tuple(beside)].set(high)


def deal_out(key, own, number, rows, amount, top, limit, lean):
    order = jax.random.permutation(key, amount)
    heavy_load, common = load_shares(amount, rows * top, limit, lean, True), load_shares(amount, rows * top, limit, lean, False)
    places = jnp.arange(amount)

    def named(tallies, offset_by):
        used = int((tallies > 0).sum())
        fixed = max(1, used // 4)
        shifted = fixed + (places - fixed + offset_by * (used - fixed)) % max(1, amount - fixed)
        return jnp.zeros((amount,), jnp.int32).at[order[jnp.where(places < fixed, places, shifted)]].set(jnp.asarray(tallies, jnp.int32))

    tallies = jnp.where(number % 4 == 0, named(heavy_load, number // 4), named(common, number - number // 4 - 1))
    mixed = jax.random.permutation(jax.random.fold_in(own, 3), amount)
    donor, taker = mixed[0:amount // 2 * 2:2], mixed[1:amount // 2 * 2:2]
    slack = jnp.minimum(tallies[donor] - 1, limit - tallies[taker]) // 2
    slack = jnp.where((donor == order[0]) | (taker == order[0]) | (tallies[taker] == 0), 0, jnp.maximum(slack, 0))
    shifted = jax.random.randint(jax.random.fold_in(own, 4), (amount // 2,), 0, 1 << 20) % (slack + 1)
    tallies = tallies.at[donor].add(-shifted).at[taker].add(shifted)
    items = jnp.searchsorted(jnp.cumsum(tallies), jnp.arange(rows * top), side="right").astype(jnp.int32)
    listing = items.reshape(top, rows).T
    listing = listing[jax.random.permutation(jax.random.fold_in(own, 1), rows)]
    offset_by = jax.random.randint(jax.random.fold_in(own, 2), (rows, 1), 0, top)
    return jnp.take_along_axis(listing, (jnp.arange(top)[None, :] + offset_by) % top, axis=1)


def load_shares(number_of, total, most, skew, full):
    loads = [(1 << 20) // math.isqrt(standing ** skew) + 1 for standing in range(1, number_of + 1)]
    largest = most if full else min(most, max(-(-total // number_of), total * loads[0] // sum(loads)))
    least = 1 if total - largest >= number_of - 1 else 0
    given, surplus = [largest] + [least] * (number_of - 1), total - largest - least * (number_of - 1)
    while surplus > 0:
        movable = [i for i in range(1, number_of) if given[i] < largest] or [i for i in range(1, number_of) if given[i] < most]
        mass, left = sum([loads[i] for i in movable]), surplus
        for i in movable:
            extra = min(most - given[i], max(1, left * loads[i] // mass), surplus)
            given[i] = given[i] + extra
            surplus = surplus - extra
    return np.array(given)


def setup_inputs(seed: int = 0) -> dict:
    key_list = jax.random.split(jax.random.key(seed), 8)
    residual = draw_residual(jax.random.fold_in(key_list[7], 71), 0)
    inverses = draw_inverses(jax.random.fold_in(key_list[7], 71), 0)
    couplings = draw_couplings(jax.random.fold_in(key_list[7], 71), 0)
    receptors = draw_receptors(jax.random.fold_in(key_list[7], 71), 0)
    owners_keys = jax.random.split(jax.random.fold_in(key_list[4], 1), GRIDS * BLOCKS_I * BLOCKS_J * R_DEV // R_DEV)
    owners_turns = jax.random.permutation(jax.random.fold_in(key_list[4], 3), GRIDS * BLOCKS_I * BLOCKS_J * R_DEV // R_DEV)
    owners = jax.vmap(lambda own, number: deal_out(jax.random.fold_in(key_list[4], 2), own, number, R_DEV, OWNERS, 1, SLOTS, 2))(owners_keys, owners_turns).reshape((GRIDS, BLOCKS_I, BLOCKS_J, R_DEV, 1))
    donors = plant(jax.random.randint(key_list[5], (GRIDS, BLOCKS_I, BLOCKS_J, R_DEV, DONORS), 0, CELLS), jax.random.fold_in(key_list[5], 1), 0, CELLS - 1).astype(jnp.int32)
    weights = draw_weights(jax.random.fold_in(key_list[7], 71), 0)
    return {"residual": residual, "inverses": inverses, "couplings": couplings, "receptors": receptors, "owners": owners, "donors": donors, "weights": weights}


def apply_block(block, vector):
    shaped = block.reshape(block.shape[:-2] + (5, 5, block.shape[-1]))
    return jnp.sum(shaped * vector[..., None, :, :], axis=-2)


def forward_grid(rhs_grid, inverse_grid, coupling_grid):
    def row_step(upper_row, inputs):
        rhs_row, inv_row, coup_row = inputs

        def cell_step(left_value, cell_inputs):
            rhs_cell, inv_cell, coup_cell, upper_cell = cell_inputs
            result = apply_block(inv_cell, rhs_cell + coup_cell[0][None] * upper_cell + coup_cell[1][None] * left_value)
            return result, result

        start = jnp.zeros(rhs_row.shape[1:], jnp.float32)
        _, row_values = lax.scan(cell_step, start, (rhs_row, inv_row, coup_row, upper_row))
        return row_values, row_values

    start_row = jnp.zeros(rhs_grid.shape[1:], jnp.float32)
    _, result = lax.scan(row_step, start_row, (rhs_grid, inverse_grid, coupling_grid))
    return result


def backward_grid(star_grid, inverse_grid, coupling_grid):
    def row_step(lower_row, inputs):
        star_row, inv_row, coup_row = inputs

        def cell_step(right_value, cell_inputs):
            star_cell, inv_cell, coup_cell, lower_cell = cell_inputs
            result = star_cell + apply_block(inv_cell, coup_cell[2][None] * lower_cell + coup_cell[3][None] * right_value)
            return result, result

        start = jnp.zeros(star_row.shape[1:], jnp.float32)
        _, row_values = lax.scan(cell_step, start, (star_row, inv_row, coup_row, lower_row), reverse=True)
        return row_values, row_values

    start_row = jnp.zeros(star_grid.shape[1:], jnp.float32)
    _, result = lax.scan(row_step, start_row, (star_grid, inverse_grid, coupling_grid), reverse=True)
    return result


def reference(residual, inverses, couplings, receptors, owners, donors, weights):
    swept_list = []
    for grid_index in range(GRIDS):
        star = forward_grid(residual[grid_index], inverses[grid_index], couplings[grid_index])
        swept_list.append(backward_grid(star, inverses[grid_index], couplings[grid_index]))
    swept = jnp.stack(swept_list)
    owner_list = owners[..., 0]
    owner_i = owner_list // BLOCKS_J
    owner_j = owner_list % BLOCKS_J
    pencil = donors // CK
    donor_i = owner_i[..., None] * CI + pencil // CJ
    donor_j = owner_j[..., None] * CJ + pencil % CJ
    donor_k = donors % CK
    grid_ids = jnp.arange(GRIDS, dtype=jnp.int32).reshape(GRIDS, 1, 1, 1, 1)
    other_grid = (1 - grid_ids) * jnp.ones_like(donors)
    values = swept[other_grid, donor_i, donor_j, :, donor_k]
    fringe = jnp.sum(values * weights[..., None], axis=-2)
    block_i = jnp.arange(BLOCKS_I, dtype=jnp.int32).reshape(1, BLOCKS_I, 1, 1)
    block_j = jnp.arange(BLOCKS_J, dtype=jnp.int32).reshape(1, 1, BLOCKS_J, 1)
    rec_pencil = receptors // CK
    rec_i = block_i * CI + rec_pencil // CJ
    rec_j = block_j * CJ + rec_pencil % CJ
    rec_k = receptors % CK
    rec_grid = grid_ids[..., 0] * jnp.ones_like(receptors)
    return swept.at[rec_grid, rec_i, rec_j, :, rec_k].set(fringe)
```

```python
import functools
import jax
import jax.numpy as jnp
from jax import lax
from jax.experimental import pallas as pl
from jax.experimental.pallas import tpu as pltpu
from jax.sharding import PartitionSpec as P

PERIOD = 8
LANES = 128
SUBS = 8
VM = pltpu.VMEM
F32 = jnp.float32


def vmem(value):
    return pltpu.with_memory_space_constraint(value, pltpu.VMEM)


def full(space):
    return pl.BlockSpec(memory_space=space)


def params(**kw):
    return pltpu.CompilerParams(vmem_limit_bytes=8 * 1024 * 1024, **kw)


def unpack_body(first, res, inv, cou, res_out, inv_out, cou_out, sem):
    del first
    for q in range(SUBS):
        lanes = pl.ds(q * LANES, LANES)
        for j in range(8):
            for n, (src, dst) in enumerate(((res, res_out), (inv, inv_out))):
                pltpu.make_async_copy(
                    src.at[:, :, j, lanes], dst.at[:, j, :, q, :], sem.at[n]
                ).start()
        pltpu.make_async_copy(cou.at[:, :, :, lanes], cou_out.at[:, :, :, q, :], sem.at[2]).start()
    for n, dst in enumerate((res_out, inv_out, cou_out)):
        pltpu.make_async_copy(dst, dst, sem.at[n]).wait()


def unpack(first, res, inv, cou):
    shapes = [(8, 8, w, SUBS, LANES) for w in (5, 25, 4)]
    hbm = lambda a: pltpu.with_memory_space_constraint(a, pltpu.HBM)
    out = pl.pallas_call(
        unpack_body,
        in_specs=[full(pl.ANY)] * 4,
        out_specs=[full(VM)] * 3,
        out_shape=[VM(shape, F32) for shape in shapes],
        scratch_shapes=[pltpu.SemaphoreType.DMA((3,))],
        compiler_params=params(),
        name="unpack",
    )(first, hbm(res), hbm(inv), hbm(cou))
    return [a.reshape((64,) + a.shape[2:]) for a in out]


def block_times(inv, p, vec):
    out = []
    for r in range(5):
        t = [inv[p, 5 * r + c] * vec[c] for c in range(5)]
        out.append(((t[0] + t[1]) + (t[2] + t[3])) + t[4])
    return out


def diagonal():
    return lax.axis_index("px") + lax.axis_index("py")


def forward_body(stage, rows_in, cols_in, res, inv, cou, star_in, rows_out, cols_out, star):
    @pl.when(diagonal() == stage)
    def _():
        rows_out[...] = rows_in[...]

        def row(i, carry):
            left = [cols_in[i, c] for c in range(5)]
            for j in range(8):
                p = i * 8 + j
                a, b = cou[p, 0], cou[p, 1]
                vec = [res[p, c] + a * rows_out[j, c] + b * left[c] for c in range(5)]
                left = block_times(inv, p, vec)
                for c in range(5):
                    rows_out[j, c] = left[c]
                    star[p, c] = left[c]
            for c in range(5):
                cols_out[i, c] = left[c]
            return carry

        lax.fori_loop(0, 8, row, 0)


def backward_body(stage, last, rows_in, cols_in, star, inv, cou, swept_in, rows_out, cols_out, swept):
    @pl.when(last - diagonal() == stage)
    def _():
        rows_out[...] = rows_in[...]

        def row(step, carry):
            i = 7 - step
            right = [cols_in[i, c] for c in range(5)]
            for j in range(7, -1, -1):
                p = i * 8 + j
                e, f = cou[p, 2], cou[p, 3]
                vec = [e * rows_out[j, c] + f * right[c] for c in range(5)]
                prod = block_times(inv, p, vec)
                right = [star[p, c] + prod[c] for c in range(5)]
                for c in range(5):
                    rows_out[j, c] = right[c]
                    swept[pl.ds(p * 64 + c, SUBS, stride=8), :] = right[c]
            for c in range(5):
                cols_out[i, c] = right[c]
            return carry

        lax.fori_loop(0, 8, row, 0)


def stage_call(body, name, faces, coeffs, state):
    face = VM(faces[0].shape, F32)
    count = len(faces) + len(coeffs)
    return pl.pallas_call(
        body,
        in_specs=[full(VM)] * (count + 1),
        out_specs=[full(VM)] * 3,
        out_shape=[face, face, VM(state.shape, F32)],
        input_output_aliases={count: 2},
        compiler_params=params(),
        name=name,
    )(*[vmem(a) for a in faces], *[vmem(a) for a in coeffs], vmem(state))


def routes(rows, cols, step, stage):
    px, py = [], []
    for i in range(rows):
        for j in range(cols):
            along = i + j if step > 0 else rows + cols - 2 - i - j
            if along % PERIOD == stage % PERIOD:
                if 0 <= i + step < rows:
                    px.append((i * cols + j, (i + step) * cols + j))
                if 0 <= j + step < cols:
                    py.append((i * cols + j, i * cols + j + step))
    return px, py


def pass_on(rows_face, cols_face, step, stage):
    px, py = routes(lax.axis_size("px"), lax.axis_size("py"), step, stage)
    return lax.ppermute(rows_face, ("px", "py"), px), lax.ppermute(cols_face, ("px", "py"), py)


def other_half():
    return (1 - lax.axis_index("grid")) * 128


def row_lane():
    return lax.broadcasted_iota(jnp.int32, (1, LANES), 1)


def request_body(owner, wanted, out, slots, count):
    out[...] = jnp.zeros_like(out)
    first = other_half()
    lane = row_lane()
    key = (lane & 63) >> 3

    def clear(o, carry):
        for n in range(8):
            count[o * 8 + n] = 0
        return carry

    lax.fori_loop(0, 16, clear, 0)

    def place(step, carry):
        for k in range(8):
            r = step * 8 + k
            o = owner[r]
            n = count[o]
            count[o] = n + 1
            slots[r] = o * 128 + n * 8
            pltpu.store(
                out.at[pl.ds(first + o, 1), :], wanted[pl.ds(r, 1), :], mask=key == n
            )
        return carry

    lax.fori_loop(0, wanted.shape[0] // 8, place, 0)


def make_request(owner, wanted):
    return pl.pallas_call(
        request_body,
        in_specs=[full(pltpu.SMEM), full(VM)],
        out_specs=[full(VM), full(pltpu.SMEM)],
        out_shape=[
            jax.ShapeDtypeStruct((256, LANES), F32),
            jax.ShapeDtypeStruct(owner.shape, jnp.int32),
        ],
        scratch_shapes=[pltpu.SMEM((128,), jnp.int32)],
        compiler_params=params(),
        name="request",
    )(owner, wanted)


def picks_body(late, asked, picks_in, picks):
    del picks_in
    first = other_half()
    lane = lax.broadcasted_iota(jnp.int32, (64, LANES), 1)

    @pl.when((diagonal() >= 12) == late)
    def _():
        def group(t, carry):
            rows = asked[pl.ds(pl.multiple_of(first + t * 8, 8), 8), :]
            turned = rows.T
            cell = turned[:64].astype(jnp.int32) & 127
            weight = turned[64:]
            for k in range(8):
                at = pl.multiple_of((t * 8 + k) * 64, 64)
                picks[pl.ds(at, 64), :] = jnp.where(
                    lane == cell[:, k : k + 1], weight[:, k : k + 1], 0.0
                )
            return carry

        lax.fori_loop(0, 16, group, 0)


def make_picks(late, asked, picks):
    return pl.pallas_call(
        functools.partial(picks_body, late),
        in_specs=[full(VM)] * 2,
        out_specs=full(VM),
        out_shape=VM(picks.shape, F32),
        input_output_aliases={1: 0},
        compiler_params=params(),
        name="picks",
    )(asked, vmem(picks))


def serve_body(index, picks, swept, out):
    out[...] = jnp.zeros_like(out)
    first = other_half()

    def pair(t, carry):
        sums = []
        for n in range(16):
            total = None
            for d in range(8):
                row = pl.multiple_of(index[t * 2 + n // 8, n % 8 * 8 + d], 8)
                pick = picks[pl.ds(t * 128 + n * 8 + d, 1), :]
                part = swept[pl.ds(row, 8), :] * pick
                total = part if total is None else total + part
            sums.append(total)
        flat = jnp.sum(jnp.concatenate(sums, axis=0).T, axis=0, keepdims=True)
        out[pl.ds(first + t * 2, 1), :] = flat
        out[pl.ds(first + t * 2 + 1, 1), :] = pltpu.roll(flat, 64, axis=1)
        return carry

    lax.fori_loop(0, 64, pair, 0)


def serve(index, picks, swept):
    return pl.pallas_call(
        serve_body,
        in_specs=[full(pltpu.SMEM), full(VM), full(VM)],
        out_specs=full(VM),
        out_shape=jax.ShapeDtypeStruct((256, LANES), F32),
        compiler_params=params(),
        name="serve",
    )(index, vmem(picks), vmem(swept))


def finish_body(receptors, slots, values, swept_in, out, swept, sem):
    lane = lax.broadcasted_iota(jnp.int32, (SUBS, LANES), 1)
    sub = lax.broadcasted_iota(jnp.int32, (SUBS, LANES), 0)

    def put(step, carry):
        for k in range(8):
            cell = receptors[step * 8 + k]
            at = slots[step * 8 + k]
            row = pl.multiple_of((cell >> 7) * 8, 8)
            new = jnp.full((SUBS, LANES), values[at], F32)
            for c in range(1, 5):
                new = jnp.where(sub == c, values[at + c], new)
            pltpu.store(swept.at[pl.ds(row, 8), :], new, mask=lane == (cell & 127))
        return carry

    lax.fori_loop(0, receptors.shape[0] // 8, put, 0)
    view = swept.reshape(8, 8, SUBS, 8, LANES)
    for q in range(SUBS):
        for j in range(8):
            pltpu.make_async_copy(
                view.at[:, j, q, pl.ds(0, 5), :],
                out.at[:, :, j, pl.ds(q * LANES, LANES)],
                sem.at[0],
            ).start()
    pltpu.make_async_copy(out, out, sem.at[0]).wait()


def finish(receptors, slots, values, swept):
    out, _ = pl.pallas_call(
        finish_body,
        in_specs=[full(pltpu.SMEM)] * 3 + [full(VM)],
        out_specs=[full(pl.ANY), full(VM)],
        out_shape=[pltpu.HBM((8, 5, 8, 1024), F32), VM(swept.shape, F32)],
        input_output_aliases={3: 1},
        scratch_shapes=[pltpu.SemaphoreType.DMA((1,))],
        compiler_params=params(),
        name="finish",
    )(receptors, slots, values, vmem(swept))
    return out


def exchange(rows):
    return lax.all_to_all(rows, ("grid", "px", "py"), split_axis=0, concat_axis=0, tiled=True)


def local(residual, inverses, couplings, receptors, owners, donors, weights):
    rows = lax.axis_size("px")
    cols = lax.axis_size("py")
    last = rows + cols - 2

    cells = jnp.tile(donors[0, 0, 0].astype(F32), (1, 8))
    wanted = jnp.concatenate([cells, jnp.tile(weights[0, 0, 0], (1, 8))], axis=1)
    request, slots = make_request(owners[0, 0, 0, :, 0], wanted)
    asked = exchange(request)
    asked_row = lax.dynamic_slice(asked, (other_half(), 0), (128, 64)).astype(jnp.int32) >> 7 << 3
    picks = jnp.zeros((8192, LANES), F32)

    by_row = lambda a: a[0].transpose(0, 2, 1, 3)
    res, inv, cou = unpack(asked_row, by_row(residual), by_row(inverses), couplings[0])

    faces = (jnp.zeros((8, 5, SUBS, LANES), F32),) * 2
    star = jnp.zeros((64, 5, SUBS, LANES), F32)
    for stage in range(last + 1):
        if stage:
            faces = pass_on(*faces, 1, stage - 1)
        *faces, star = stage_call(
            functools.partial(forward_body, stage), "forward", faces, (res, inv, cou), star
        )
        if stage in (2, 20):
            picks = make_picks(stage == 2, asked, picks)
    faces = (jnp.zeros((8, 5, SUBS, LANES), F32),) * 2
    swept = jnp.zeros((64 * SUBS * 8, LANES), F32)
    for stage in range(last + 1):
        if stage:
            faces = pass_on(*faces, -1, stage - 1)
        *faces, swept = stage_call(
            functools.partial(backward_body, stage, last), "backward", faces, (star, inv, cou), swept
        )

    answers = exchange(serve(asked_row, picks, swept)).reshape(256 * LANES)
    answers = lax.dynamic_slice(answers, (other_half() * LANES,), (128 * LANES,))
    out = finish(receptors[0, 0, 0], slots, answers, swept)
    return out.transpose(0, 2, 1, 3)[None]


def solution(mesh):
    placed = (
        P("grid", "px", "py", None, None),
        P("grid", "px", "py", None, None),
        P("grid", "px", "py", None, None),
        P("grid", "px", "py", None),
        P("grid", "px", "py", None, None),
        P("grid", "px", "py", None, None),
        P("grid", "px", "py", None, None),
    )
    return jax.shard_map(
        local,
        mesh=mesh,
        in_specs=placed,
        out_specs=P("grid", "px", "py", None, None),
        check_vma=False,
    )
```

```python
import functools
import jax
import jax.numpy as jnp
from jax import lax
from jax.experimental import pallas as pl
from jax.experimental.pallas import tpu as pltpu
from jax.sharding import PartitionSpec as P

PERIOD = 8
PARTS = 2
LAG = 2
LANES = 128
SUBS = 8
VM = pltpu.VMEM
F32 = jnp.float32


def vmem(value):
    return pltpu.with_memory_space_constraint(value, pltpu.VMEM)


def full(space):
    return pl.BlockSpec(memory_space=space)


def params(**kw):
    return pltpu.CompilerParams(vmem_limit_bytes=8 * 1024 * 1024, **kw)


def prepare_body(
    owner, donors, weights, res, inv, cou, out, slots, res_out, inv_out, cou_out, wanted, count, sem
):
    for q in range(SUBS):
        lanes = pl.ds(q * LANES, LANES)
        for j in range(8):
            for n, (src, dst) in enumerate(((res, res_out), (inv, inv_out))):
                pltpu.make_async_copy(
                    src.at[:, :, j, lanes], dst.at[:, j, :, q, :], sem.at[n]
                ).start()
        pltpu.make_async_copy(cou.at[:, :, :, lanes], cou_out.at[:, :, :, q, :], sem.at[2]).start()

    out[...] = jnp.zeros_like(out)
    wanted[...] = jnp.concatenate([donors[...].astype(F32)] * 8 + [weights[...]] * 8, axis=0).T
    first = other_half()
    key = (row_lane() & 63) >> 3

    def clear(step, carry):
        for n in range(8):
            count[step * 8 + n] = 0
        return carry

    lax.fori_loop(0, 16, clear, 0)

    def place(step, carry):
        for k in range(8):
            r = step * 8 + k
            o = owner[r]
            n = count[o]
            count[o] = n + 1
            slots[r] = o * 128 + n * 8
            pltpu.store(
                out.at[pl.ds(first + o, 1), :], wanted[pl.ds(r, 1), :], mask=key == n
            )
        return carry

    lax.fori_loop(0, wanted.shape[0] // 8, place, 0)
    for n, dst in enumerate((res_out, inv_out, cou_out)):
        pltpu.make_async_copy(dst, dst, sem.at[n]).wait()


def prepare(owner, donors, weights, res, inv, cou):
    shapes = [(8, 8, w, SUBS, LANES) for w in (5, 25, 4)]
    hbm = lambda a: pltpu.with_memory_space_constraint(a, pltpu.HBM)
    request, slots, *rest = pl.pallas_call(
        prepare_body,
        in_specs=[full(pltpu.SMEM), full(VM), full(VM)] + [full(pl.ANY)] * 3,
        out_specs=[full(VM), full(pltpu.SMEM)] + [full(VM)] * 3,
        out_shape=[
            VM((256, LANES), F32),
            jax.ShapeDtypeStruct(owner.shape, jnp.int32),
        ]
        + [VM(shape, F32) for shape in shapes],
        scratch_shapes=[
            pltpu.VMEM((512, LANES), F32),
            pltpu.SMEM((128,), jnp.int32),
            pltpu.SemaphoreType.DMA((3,)),
        ],
        compiler_params=params(),
        name="prepare",
    )(owner, donors, weights, hbm(res), hbm(inv), hbm(cou))
    return request, slots, [a.reshape((64,) + a.shape[2:]) for a in rest]


def block_times(inv, p, part, vec):
    out = []
    for r in range(5):
        t = [inv[p, 5 * r + c, part, :] * vec[c] for c in range(5)]
        out.append(((t[0] + t[1]) + (t[2] + t[3])) + t[4])
    return out


def diagonal():
    return lax.axis_index("px") + lax.axis_index("py")


def parts_due(stage, arrival):
    def call(work):
        for n in range(PARTS):
            size = SUBS // PARTS

            @pl.when(arrival + LAG * n == stage)
            def _():
                work(n * size, slice(n * size, (n + 1) * size))

    return call


def forward_body(stage, rows_in, cols_in, res, inv, cou, star_in, rows_out, cols_out, star):
    @parts_due(stage, diagonal())
    def _(start, part):
        rows_out[...] = rows_in[...]

        def row(i, carry):
            left = [cols_in[i, c] for c in range(5)]
            for j in range(8):
                p = i * 8 + j
                a, b = cou[p, 0, part, :], cou[p, 1, part, :]
                vec = [res[p, c, part, :] + a * rows_out[j, c] + b * left[c] for c in range(5)]
                left = block_times(inv, p, part, vec)
                for c in range(5):
                    rows_out[j, c] = left[c]
                    star[p, c, part, :] = left[c]
            for c in range(5):
                cols_out[i, c] = left[c]
            return carry

        lax.fori_loop(0, 8, row, 0)


def backward_body(stage, last, rows_in, cols_in, star, inv, cou, swept_in, rows_out, cols_out, swept):
    @parts_due(stage, last - diagonal())
    def _(start, part):
        rows_out[...] = rows_in[...]

        def row(step, carry):
            i = 7 - step
            right = [cols_in[i, c] for c in range(5)]
            for j in range(7, -1, -1):
                p = i * 8 + j
                e, f = cou[p, 2, part, :], cou[p, 3, part, :]
                vec = [e * rows_out[j, c] + f * right[c] for c in range(5)]
                prod = block_times(inv, p, part, vec)
                right = [star[p, c, part, :] + prod[c] for c in range(5)]
                for c in range(5):
                    rows_out[j, c] = right[c]
                    swept[pl.ds(p * 64 + start * 8 + c, SUBS // PARTS, stride=8), :] = right[c]
            for c in range(5):
                cols_out[i, c] = right[c]
            return carry

        lax.fori_loop(0, 8, row, 0)


def stage_call(body, name, faces, coeffs, state, after=()):
    face = VM(faces[0].shape, F32)
    count = len(faces) + len(coeffs)

    def run(*refs):
        body(*refs[: count + 1], *refs[count + 1 + len(after) :])

    return pl.pallas_call(
        run,
        in_specs=[full(VM)] * (count + 1) + [full(pl.ANY)] * len(after),
        out_specs=[full(VM)] * 3,
        out_shape=[face, face, VM(state.shape, F32)],
        input_output_aliases={count: 2},
        compiler_params=params(),
        name=name,
    )(*[vmem(a) for a in faces], *[vmem(a) for a in coeffs], vmem(state), *after)


def routes(rows, cols, step, stage):
    px, py = [], []
    for i in range(rows):
        for j in range(cols):
            along = i + j if step > 0 else rows + cols - 2 - i - j
            if any((stage - LAG * n - along) % PERIOD == 0 for n in range(PARTS)):
                if 0 <= i + step < rows:
                    px.append((i * cols + j, (i + step) * cols + j))
                if 0 <= j + step < cols:
                    py.append((i * cols + j, i * cols + j + step))
    return px, py


def pass_on(rows_face, cols_face, step, stage):
    px, py = routes(lax.axis_size("px"), lax.axis_size("py"), step, stage)
    return lax.ppermute(rows_face, ("px", "py"), px), lax.ppermute(cols_face, ("px", "py"), py)


def other_half():
    return (1 - lax.axis_index("grid")) * 128


def row_lane():
    return lax.broadcasted_iota(jnp.int32, (1, LANES), 1)


def fill_picks(asked, picks):
    first = other_half()
    lane = lax.broadcasted_iota(jnp.int32, (64, LANES), 1)

    def group(t, carry):
        turned = asked[pl.ds(pl.multiple_of(first + t * 8, 8), 8), :].T
        cell = turned[:64].astype(jnp.int32) & 127
        weight = turned[64:]
        for k in range(8):
            at = pl.multiple_of((t * 8 + k) * 64, 64)
            picks[pl.ds(at, 64), :] = jnp.where(
                lane == cell[:, k : k + 1], weight[:, k : k + 1], 0.0
            )
        return carry

    lax.fori_loop(0, 16, group, 0)


def late_body(asked, picks):
    @pl.when(diagonal() >= 12)
    def _():
        fill_picks(asked, picks)


def early_body(asked, picks_in, picks, rows):
    del picks_in
    first = pl.multiple_of(other_half(), 128)
    rows[...] = asked[pl.ds(first, 128), :].astype(jnp.int32) >> 7 << 3

    @pl.when(diagonal() < 12)
    def _():
        fill_picks(asked, picks)


def late_picks(asked):
    return pl.pallas_call(
        late_body,
        in_specs=[full(VM)],
        out_specs=full(VM),
        out_shape=VM((8192, LANES), F32),
        compiler_params=params(),
        name="late",
    )(vmem(asked))


def early_picks(asked, picks):
    return pl.pallas_call(
        early_body,
        in_specs=[full(VM)] * 2,
        out_specs=[full(VM)] * 2,
        out_shape=[VM(picks.shape, F32), VM((128, LANES), jnp.int32)],
        input_output_aliases={1: 0},
        compiler_params=params(),
        name="early",
    )(vmem(asked), vmem(picks))


def serve_body(index, picks, swept, out, sums):
    out[...] = jnp.zeros_like(out)
    first = other_half()

    def write(t):
        flat = jnp.sum(sums[...].T, axis=0, keepdims=True)
        out[pl.ds(first + t * 2, 1), :] = flat
        out[pl.ds(first + t * 2 + 1, 1), :] = pltpu.roll(flat, 64, axis=1)

    def pair(t, carry):
        write(jnp.maximum(t - 1, 0))
        for n in range(16):
            total = None
            for d in range(8):
                row = pl.multiple_of(index[t * 2 + n // 8, n % 8 * 8 + d], 8)
                pick = picks[pl.ds(t * 128 + n * 8 + d, 1), :]
                part = swept[pl.ds(row, 8), :] * pick
                total = part if total is None else total + part
            sums[pl.ds(n * 8, 8), :] = total
        return carry

    sums[...] = jnp.zeros_like(sums)
    lax.fori_loop(0, 64, pair, 0)
    write(63)


def serve(index, picks, swept):
    return pl.pallas_call(
        serve_body,
        in_specs=[full(pltpu.SMEM), full(VM), full(VM)],
        out_specs=full(VM),
        out_shape=jax.ShapeDtypeStruct((256, LANES), F32),
        scratch_shapes=[pltpu.VMEM((LANES, LANES), F32)],
        compiler_params=params(),
        name="serve",
    )(index, vmem(picks), vmem(swept))


def finish_body(receptors, slots, values, swept_in, out, swept, sem):
    lane = lax.broadcasted_iota(jnp.int32, (SUBS, LANES), 1)
    sub = lax.broadcasted_iota(jnp.int32, (SUBS, LANES), 0)

    def put(step, carry):
        for k in range(8):
            cell = receptors[step * 8 + k]
            at = slots[step * 8 + k]
            row = pl.multiple_of((cell >> 7) * 8, 8)
            new = jnp.full((SUBS, LANES), values[at], F32)
            for c in range(1, 5):
                new = jnp.where(sub == c, values[at + c], new)
            pltpu.store(swept.at[pl.ds(row, 8), :], new, mask=lane == (cell & 127))
        return carry

    lax.fori_loop(0, receptors.shape[0] // 8, put, 0)
    view = swept.reshape(8, 8, SUBS, 8, LANES)
    for q in range(SUBS):
        for j in range(8):
            pltpu.make_async_copy(
                view.at[:, j, q, pl.ds(0, 5), :],
                out.at[:, :, j, pl.ds(q * LANES, LANES)],
                sem.at[0],
            ).start()
    pltpu.make_async_copy(out, out, sem.at[0]).wait()


def finish(receptors, slots, values, swept):
    out, _ = pl.pallas_call(
        finish_body,
        in_specs=[full(pltpu.SMEM)] * 3 + [full(VM)],
        out_specs=[full(pl.ANY), full(VM)],
        out_shape=[pltpu.HBM((8, 5, 8, 1024), F32), VM(swept.shape, F32)],
        input_output_aliases={3: 1},
        scratch_shapes=[pltpu.SemaphoreType.DMA((1,))],
        compiler_params=params(),
        name="finish",
    )(receptors, slots, values, vmem(swept))
    return out


def exchange(rows):
    return lax.all_to_all(rows, ("grid", "px", "py"), split_axis=0, concat_axis=0, tiled=True)


def local(residual, inverses, couplings, receptors, owners, donors, weights):
    rows = lax.axis_size("px")
    cols = lax.axis_size("py")
    last = rows + cols - 2

    by_row = lambda a: a[0].transpose(0, 2, 1, 3)
    request, slots, (res, inv, cou) = prepare(
        owners[0, 0, 0, :, 0],
        donors[0, 0, 0].T,
        weights[0, 0, 0].T,
        by_row(residual),
        by_row(inverses),
        couplings[0],
    )
    asked = exchange(request)

    faces = (jnp.zeros((8, 5, SUBS // PARTS, LANES), F32),) * 2
    star = jnp.zeros((64, 5, SUBS, LANES), F32)
    for stage in range(last + 1 + LAG * (PARTS - 1)):
        if stage:
            faces = pass_on(*faces, 1, stage - 1)
        *faces, star = stage_call(
            functools.partial(forward_body, stage),
            "forward",
            faces,
            (res, inv, cou),
            star,
            (picks,) if stage == 5 else (),
        )
        if stage == 4:
            picks = late_picks(asked)
        if stage == 20:
            picks, asked_row = early_picks(asked, picks)
    faces = (jnp.zeros((8, 5, SUBS // PARTS, LANES), F32),) * 2
    swept = jnp.zeros((64 * SUBS * 8, LANES), F32)
    for stage in range(last + 1 + LAG * (PARTS - 1)):
        if stage:
            faces = pass_on(*faces, -1, stage - 1)
        *faces, swept = stage_call(
            functools.partial(backward_body, stage, last),
            "backward",
            faces,
            (star, inv, cou),
            swept,
            () if stage else (asked_row,),
        )

    answers = exchange(serve(asked_row, picks, swept)).reshape(256 * LANES)
    answers = lax.dynamic_slice(answers, (other_half() * LANES,), (128 * LANES,))
    out = finish(receptors[0, 0, 0], slots, answers, swept)
    return out.transpose(0, 2, 1, 3)[None]


def solution(mesh):
    placed = (
        P("grid", "px", "py", None, None),
        P("grid", "px", "py", None, None),
        P("grid", "px", "py", None, None),
        P("grid", "px", "py", None),
        P("grid", "px", "py", None, None),
        P("grid", "px", "py", None, None),
        P("grid", "px", "py", None, None),
    )
    return jax.shard_map(
        local,
        mesh=mesh,
        in_specs=placed,
        out_specs=P("grid", "px", "py", None, None),
        check_vma=False,
    )
```
